32 devices in a mesh: inst: 2 (over x), qy: 4 (over z), qx: 4 (over y, core).
Axes of the slice: x: 2, y: 2, z: 4, core: 2. Of those that a mesh axis runs over, the one named last changes fastest.
Arguments:
- cost_diag: float32 [8388608], P(('inst', 'qx', 'qy')), parts along dimension 0
- gammas: float32 [4], replicated
- betas: float32 [4], replicated
Outputs:
- output 1: float32 [2], P('inst'), parts along dimension 0
- output 2: float32 [8388608], P(('inst', 'qx', 'qy')), parts along dimension 0
- output 3: float32 [8388608], P(('inst', 'qx', 'qy')), parts along dimension 0
There are 2 independent parts. The reference program is written for one: setup_inputs(seed, part) draws one part's arguments, and reference() takes and returns one part's arrays. A program takes and returns all parts, laid end to end along the dimension named above; an argument that names none is the same for every part.
All inputs are finite; a program needn't handle non-finite values.
Results may differ from the reference program's by a relative error of at most 0.001.
Values sent between devices are 32-bit elements.
A program may use at most 1 GiB of HBM per device.

```python
import math
import jax
import jax.numpy as jnp
from jax import lax

STATE = 4194304
LAYERS = 4
DEGREE = 3

QUBITS = int(math.log2(STATE))
EDGES = DEGREE * QUBITS // 2


def setup_inputs(seed: int = 0, part: int = 0) -> dict:
    base_key = jax.random.key(seed)
    part_key = jax.random.fold_in(base_key, part)
    key_offset, key_weight = jax.random.split(part_key)
    first_node = jnp.arange(EDGES, dtype=jnp.int32) % QUBITS
    offsets = jax.random.randint(key_offset, (EDGES,), 1, QUBITS, dtype=jnp.int32)
    second_node = (first_node + offsets) % QUBITS
    weights = jax.random.uniform(key_weight, (EDGES,), jnp.float32, 0.5, 1.5) * (2.0 / math.sqrt(EDGES))
    basis_index = jnp.arange(STATE, dtype=jnp.int32)

    def add_edge(edge_id, cost_acc):
        cut_bit = ((basis_index >> first_node[edge_id]) ^ (basis_index >> second_node[edge_id])) & 1
        return cost_acc + weights[edge_id] * cut_bit.astype(jnp.float32)

    cost_diag = lax.fori_loop(0, EDGES, add_edge, jnp.zeros((STATE,), jnp.float32))
    key_gamma, key_beta = jax.random.split(jax.random.key(seed + 1))
    gammas = jax.random.uniform(key_gamma, (LAYERS,), jnp.float32, 0.3, 1.0)
    betas = jax.random.uniform(key_beta, (LAYERS,), jnp.float32, 0.4, 1.2)
    return {'cost_diag': cost_diag, 'gammas': gammas, 'betas': betas}


def apply_mixer(state_re, state_im, cos_half, sin_half):
    for qubit_id in range(QUBITS):
        view_shape = (STATE >> (qubit_id + 1), 2, 1 << qubit_id)
        view_re = state_re.reshape(view_shape)
        view_im = state_im.reshape(view_shape)
        flip_re = jnp.flip(view_re, axis=1)
        flip_im = jnp.flip(view_im, axis=1)
        state_re = (cos_half * view_re + sin_half * flip_im).reshape(STATE)
        state_im = (cos_half * view_im - sin_half * flip_re).reshape(STATE)
    return state_re, state_im


def reference(cost_diag, gammas, betas):
    def layer_step(scan_carry, angles):
        state_re, state_im = scan_carry
        layer_gamma, layer_beta = angles
        phase_angle = layer_gamma * cost_diag
        cos_phase = jnp.cos(phase_angle)
        sin_phase = jnp.sin(phase_angle)
        new_re = state_re * cos_phase + state_im * sin_phase
        new_im = state_im * cos_phase - state_re * sin_phase
        cos_half = jnp.cos(0.5 * layer_beta)
        sin_half = jnp.sin(0.5 * layer_beta)
        return apply_mixer(new_re, new_im, cos_half, sin_half), None

    init_state = (jnp.ones((STATE,), jnp.float32), jnp.zeros((STATE,), jnp.float32))
    final_state, layer_outs = lax.scan(layer_step, init_state, (gammas, betas))
    state_re, state_im = final_state
    energy = jnp.sum(cost_diag * (state_re * state_re + state_im * state_im)) / STATE
    return energy.reshape(1), state_re, state_im
```

```python
import functools
import jax
import jax.numpy as jnp
from jax import lax
from jax.experimental import pallas as pl
from jax.experimental.pallas import tpu as pltpu
from jax.sharding import PartitionSpec as P

MESH = pl.DeviceIdType.MESH
LAYERS = 4
BLOCKS = 16
ROWS = 128
LANES = 128
GROUPS = ((2, 3, 6, 7), (10, 11, 14, 15), (1, 5, 9, 13), (12, 8, 4, 0))
HIGHEST = lax.Precision.HIGHEST


def flip(bits, mask):
    new = [1 - b if (mask >> i) & 1 else b for i, b in enumerate(bits)]
    qy = new[0] + 2 * new[1]
    qx = new[2] + 2 * new[3]
    return 4 * qx + qy, {'qx': qx, 'qy': qy}


def gates(vals, cos_half, sin_half):
    vals = list(vals)
    for bit in range(4):
        step = 1 << bit
        for low in range(BLOCKS):
            if low & step:
                continue
            (ar, ai), (br, bi) = vals[low], vals[low + step]
            vals[low] = (cos_half * ar + sin_half * bi, cos_half * ai - sin_half * br)
            vals[low + step] = (cos_half * br + sin_half * ai, cos_half * bi - sin_half * ar)
    return vals


def kernel(size, cost_ref, gam_ref, bet_ref, en_ref, re_ref, im_ref, cost_b, work, snd, rcv, tab, mix, half, part,
           cs_sem, cr_sem, ss_sem, sr_sem, es_sem, er_sem):
    qx, qy = lax.axis_index('qx'), lax.axis_index('qy')
    bits = [lax.rem(qy, 2), lax.div(qy, 2), lax.rem(qx, 2), lax.div(qx, 2)]
    me = 4 * qx + qy

    barrier = pltpu.get_barrier_semaphore()
    for mask in range(1, BLOCKS):
        pl.semaphore_signal(barrier, inc=1, device_id=flip(bits, mask)[1], device_id_type=MESH)
    pl.semaphore_wait(barrier, BLOCKS - 1)

    def copies(src, dst, send_sem, recv_sem, mask):
        peer, where = flip(bits, mask)
        return pltpu.make_async_remote_copy(src_ref=src(peer), dst_ref=dst, send_sem=send_sem.at[mask],
                                            recv_sem=recv_sem.at[mask], device_id=where, device_id_type=MESH)

    cost_copies = [copies(lambda peer: cost_ref.at[peer], cost_b.at[me], cs_sem, cr_sem, mask)
                   for group in GROUPS for mask in group if mask]
    for copy in cost_copies:
        copy.start()
    cost_b[me] = cost_ref[me]

    ri = lax.broadcasted_iota(jnp.int32, (ROWS, LANES), 0)
    ci = lax.broadcasted_iota(jnp.int32, (ROWS, LANES), 1)
    diff = ri ^ ci
    dist = diff & 1
    for i in range(1, 7):
        dist = dist + ((diff >> i) & 1)
    for layer in range(LAYERS):
        angle = jnp.full((8, LANES), bet_ref[layer], jnp.float32) * 0.5
        half[layer, 0] = jnp.cos(angle)
        half[layer, 1] = jnp.sin(angle)
        c = half[layer, 0, 0:1, :]
        s = half[layer, 1, 0:1, :]
        cp, sp = [jnp.ones_like(c)], [jnp.ones_like(s)]
        for _ in range(7):
            cp.append(cp[-1] * c)
            sp.append(sp[-1] * s)
        real = jnp.zeros((ROWS, LANES), jnp.float32)
        imag = jnp.zeros((ROWS, LANES), jnp.float32)
        for d in range(8):
            term = cp[7 - d] * sp[d]
            if d % 4 in (1, 2):
                term = -term
            term = jnp.broadcast_to(term, (ROWS, LANES))
            if d % 2 == 0:
                real = jnp.where(dist == d, term, real)
            else:
                imag = jnp.where(dist == d, term, imag)
        mix[layer, 0:128, 0:128] = real
        mix[layer, 0:128, 128:256] = imag
        mix[layer, 128:256, 0:128] = -imag
        mix[layer, 128:256, 128:256] = real

    def table(layer, load):
        gamma = gam_ref[layer]

        def fill(k, carry):
            angle = gamma * load(k)
            tab[layer, k, :, 0:128] = jnp.cos(angle)
            tab[layer, k, :, 128:256] = jnp.sin(angle)
            return carry

        lax.fori_loop(0, BLOCKS, fill, 0)

    def top_first():
        c, s = half[0, 0], half[0, 1]

        def rows(r, carry):
            at = pl.ds(pl.multiple_of(r * 8, 8), 8)
            vals = [(tab[0, k, at, 0:128], -tab[0, k, at, 128:256]) for k in range(BLOCKS)]
            vals = gates(vals, c, s)
            for k in range(BLOCKS):
                work[k, at, 0:128] = vals[k][0]
                work[k, at, 128:256] = vals[k][1]
            return carry

        lax.fori_loop(0, ROWS // 8, rows, 0)

    def top(layer):
        c0, s0, c1, s1 = half[layer - 1, 0], half[layer - 1, 1], half[layer, 0], half[layer, 1]

        def rows(r, carry):
            at = pl.ds(pl.multiple_of(r * 8, 8), 8)
            vals = [(rcv[layer - 1, k, at, 0:128], rcv[layer - 1, k, at, 128:256]) for k in range(BLOCKS)]
            vals = gates(vals, c0, s0)
            for k in range(BLOCKS):
                re, im = vals[k]
                pc, ps = tab[layer, k, at, 0:128], tab[layer, k, at, 128:256]
                vals[k] = (re * pc + im * ps, im * pc - re * ps)
            vals = gates(vals, c1, s1)
            for k in range(BLOCKS):
                work[k, at, 0:128] = vals[k][0]
                work[k, at, 128:256] = vals[k][1]
            return carry

        lax.fori_loop(0, ROWS // 8, rows, 0)

    def low_and_send(layer):
        started = []
        for group in GROUPS:
            index = [flip(bits, mask)[0] for mask in group]
            x = jnp.concatenate([work[k] for k in index], axis=0)
            y = jnp.dot(x, mix[layer], precision=HIGHEST, preferred_element_type=jnp.float32)
            y = jnp.concatenate(
                [jnp.concatenate([y[i * 128:(i + 1) * 128, 0:128].T, y[i * 128:(i + 1) * 128, 128:256].T], axis=1)
                 for i in range(len(group))], axis=0)
            y = jnp.dot(y, mix[layer], precision=HIGHEST, preferred_element_type=jnp.float32)
            for i, mask in enumerate(group):
                if mask:
                    snd[layer, index[i]] = y[i * 128:(i + 1) * 128]
                else:
                    rcv[layer, me] = y[i * 128:(i + 1) * 128]
            for mask in group:
                if mask:
                    copy = copies(lambda peer: snd.at[layer, peer], rcv.at[layer, me], ss_sem.at[layer],
                                  sr_sem.at[layer], mask)
                    copy.start()
                    started.append(copy)
        return started

    table(0, lambda k: cost_ref[k])
    top_first()
    pending = low_and_send(0)
    table(2, lambda k: cost_ref[k])
    for copy in cost_copies:
        copy.wait()

    def turned(k):
        return cost_b[k].T

    table(1, turned)
    for layer in range(1, LAYERS):
        if layer == 2:
            table(3, turned)
        for copy in pending:
            copy.wait()
        top(layer)
        pending = low_and_send(layer)
    for copy in pending:
        copy.wait()

    last = LAYERS - 1
    c, s = half[last, 0], half[last, 1]

    def finish(r, acc):
        at = pl.ds(pl.multiple_of(r * 8, 8), 8)
        vals = gates([(rcv[last, k, at, 0:128], rcv[last, k, at, 128:256]) for k in range(BLOCKS)], c, s)
        for k in range(BLOCKS):
            re, im = vals[k]
            re_ref[k, at, :] = re
            im_ref[k, at, :] = im
            acc = acc + cost_ref[k, at, :] * (re * re + im * im)
        return acc

    part[me] = lax.fori_loop(0, ROWS // 8, finish, jnp.zeros((8, LANES), jnp.float32))
    sums = [copies(lambda peer: part.at[me], part.at[me], es_sem, er_sem, mask) for mask in range(1, BLOCKS)]
    for copy in sums:
        copy.start()
    for copy in sums:
        copy.wait()
    total = part[0]
    for k in range(1, BLOCKS):
        total = total + part[k]
    en_ref[0] = jnp.sum(total) / size


def solution(mesh):
    state_spec = P(('inst', 'qx', 'qy'))

    def device_body(cost_local, gammas, betas):
        local_len = cost_local.shape[0]
        size = local_len * mesh.shape['qx'] * mesh.shape['qy']
        block = (BLOCKS, ROWS, LANES)
        pair = (BLOCKS, ROWS, 2 * LANES)
        vmem = pl.BlockSpec(memory_space=pltpu.VMEM)
        smem = pl.BlockSpec(memory_space=pltpu.SMEM)
        dma = pltpu.SemaphoreType.DMA
        energy, state_re, state_im = pl.pallas_call(
            functools.partial(kernel, size),
            out_shape=(jax.ShapeDtypeStruct((1,), jnp.float32), jax.ShapeDtypeStruct(block, jnp.float32),
                       jax.ShapeDtypeStruct(block, jnp.float32)),
            in_specs=[vmem, smem, smem],
            out_specs=(smem, vmem, vmem),
            scratch_shapes=[
                pltpu.VMEM(block, jnp.float32),
                pltpu.VMEM(pair, jnp.float32),
                pltpu.VMEM((LAYERS,) + pair, jnp.float32),
                pltpu.VMEM((LAYERS,) + pair, jnp.float32),
                pltpu.VMEM((LAYERS,) + pair, jnp.float32),
                pltpu.VMEM((LAYERS, 2 * LANES, 2 * LANES), jnp.float32),
                pltpu.VMEM((LAYERS, 2, 8, LANES), jnp.float32),
                pltpu.VMEM((BLOCKS, 8, LANES), jnp.float32),
                dma((BLOCKS,)), dma((BLOCKS,)),
                dma((LAYERS, BLOCKS)), dma((LAYERS, BLOCKS)),
                dma((BLOCKS,)), dma((BLOCKS,)),
            ],
            compiler_params=pltpu.CompilerParams(collective_id=0, has_side_effects=True),
            name='qaoa',
        )(cost_local.reshape(block), gammas, betas)
        return energy, state_re.reshape(local_len), state_im.reshape(local_len)

    return jax.shard_map(device_body, mesh=mesh, in_specs=(state_spec, P(), P()),
                         out_specs=(P('inst'), state_spec, state_spec), check_vma=False)
```

```python
import functools
import jax
import jax.numpy as jnp
from jax import lax
from jax.experimental import pallas as pl
from jax.experimental.pallas import tpu as pltpu
from jax.sharding import PartitionSpec as P

MESH = pl.DeviceIdType.MESH
LAYERS = 4
BLOCKS = 16
ROWS = 128
HALF = ROWS // 2
LANES = 128
CHUNKS = 8
STEP = BLOCKS // CHUNKS
GROUPS = ((2, 4, 8, 14), (6, 10, 12, 15), (3, 5, 9, 7), (11, 13, 1, 0))
PAIRS = ((2, 3), (6, 7), (4, 5), (0, 1))
HIGHEST = lax.Precision.HIGHEST


def gates(vals, cos_half, sin_half):
    vals = list(vals)
    for bit in range(4):
        step = 1 << bit
        for low in range(BLOCKS):
            if low & step:
                continue
            (ar, ai), (br, bi) = vals[low], vals[low + step]
            vals[low] = (cos_half * ar + sin_half * bi, cos_half * ai - sin_half * br)
            vals[low + step] = (cos_half * br + sin_half * ai, cos_half * bi - sin_half * ar)
    return vals


def kernel(size, cost_ref, gam_ref, bet_ref, en_ref, re_ref, im_ref, both, far, cost_b, work, snd, rcv, tab, mix, half,
           part, xs_sem, xr_sem, zs_sem, zr_sem, cs_sem, cr_sem, ss_sem, sr_sem, fs_sem, fr_sem, es_sem, er_sem):
    x, qx, qy = lax.axis_index('inst'), lax.axis_index('qx'), lax.axis_index('qy')
    core, y = lax.rem(qx, 2), lax.div(qx, 2)
    z0, h = lax.rem(qy, 2), lax.div(qy, 2)
    home = 1 - (x + h - 2 * x * h)
    cid = core + 2 * z0 + 4 * y + 8 * x

    def pick(bit, mask, i):
        return 1 - bit if (mask >> i) & 1 else bit

    def cube_peer(mask):
        c, z, v, u = pick(core, mask, 0), pick(z0, mask, 1), pick(y, mask, 2), pick(x, mask, 3)
        return c + 2 * z + 4 * v + 8 * u, {'inst': u, 'qx': 2 * v + c, 'qy': 2 * h + z}

    def plane_peer(mask, inst):
        c, z, v, t = pick(core, mask, 0), pick(z0, mask, 1), pick(y, mask, 2), pick(h, mask, 3)
        return c + 2 * z + 4 * v, t, {'inst': inst, 'qx': 2 * v + c, 'qy': 2 * t + z}

    barrier = pltpu.get_barrier_semaphore()
    for mask in range(2 * BLOCKS):
        if mask:
            inst = pick(x, mask, 4)
            pl.semaphore_signal(barrier, inc=1, device_id=plane_peer(mask, inst)[2], device_id_type=MESH)
    pl.semaphore_wait(barrier, 2 * BLOCKS - 1)

    def remote(src, dst, send_sem, recv_sem, where):
        return pltpu.make_async_remote_copy(src_ref=src, dst_ref=dst, send_sem=send_sem, recv_sem=recv_sem,
                                            device_id=where, device_id_type=MESH)

    here = pl.ds(pl.multiple_of(HALF * x, HALF), HALF)
    there = pl.ds(pl.multiple_of(HALF * (1 - x), HALF), HALF)
    slot_h = pl.ds(pl.multiple_of(HALF * h, HALF), HALF)
    slot_f = pl.ds(pl.multiple_of(HALF * (1 - h), HALF), HALF)
    x_copies, z_copies = [], []
    for j in range(CHUNKS):
        at = pl.ds(STEP * j, STEP)
        x_copies.append(remote(cost_ref.at[at, there], both.at[0, at], xs_sem.at[j], xr_sem.at[j],
                               {'inst': 1 - x, 'qx': qx, 'qy': qy}))
        z_copies.append(remote(both.at[1 - home, at], far.at[at], zs_sem.at[j], zr_sem.at[j],
                               {'inst': x, 'qx': qx, 'qy': 2 * (1 - h) + z0}))
    for copy in x_copies:
        copy.start()
    both[1] = cost_ref[:, here, :]

    ri = lax.broadcasted_iota(jnp.int32, (ROWS, LANES), 0)
    ci = lax.broadcasted_iota(jnp.int32, (ROWS, LANES), 1)
    diff = ri ^ ci
    dist = diff & 1
    for i in range(1, 7):
        dist = dist + ((diff >> i) & 1)
    for layer in range(LAYERS):
        angle = jnp.full((8, LANES), bet_ref[layer], jnp.float32) * 0.5
        half[layer, 0] = jnp.cos(angle)
        half[layer, 1] = jnp.sin(angle)
        c = half[layer, 0, 0:1, :]
        s = half[layer, 1, 0:1, :]
        cp, sp = [jnp.ones_like(c)], [jnp.ones_like(s)]
        for _ in range(7):
            cp.append(cp[-1] * c)
            sp.append(sp[-1] * s)
        real = jnp.zeros((ROWS, LANES), jnp.float32)
        imag = jnp.zeros((ROWS, LANES), jnp.float32)
        for d in range(8):
            term = cp[7 - d] * sp[d]
            if d % 4 in (1, 2):
                term = -term
            term = jnp.broadcast_to(term, (ROWS, LANES))
            if d % 2 == 0:
                real = jnp.where(dist == d, term, real)
            else:
                imag = jnp.where(dist == d, term, imag)
        mix[layer, 0:128, 0:128] = real
        mix[layer, 0:128, 128:256] = imag
        mix[layer, 128:256, 0:128] = -imag
        mix[layer, 128:256, 128:256] = real

    def table(layer, load, rows, first, count):
        gamma = gam_ref[layer]

        def fill(k, carry):
            angle = gamma * load(k)
            tab[layer, k, rows, 0:128] = jnp.cos(angle)
            tab[layer, k, rows, 128:256] = jnp.sin(angle)
            return carry

        lax.fori_loop(first, first + count, fill, 0)

    def block_to(d):
        return {'inst': d >> 3, 'qx': 2 * ((d >> 2) & 1) + (d & 1), 'qy': 2 * h + ((d >> 1) & 1)}

    def pass_on(src, d, rows, which):
        @pl.when(cid != d)
        def _():
            remote(src.at[d], cost_b.at[cid, rows], cs_sem.at[which, d], cr_sem.at[which, cid], block_to(d)).start()

    def keep(k):
        return both[home, k]

    def distant(k):
        return far[k]

    for j in range(CHUNKS):
        x_copies[j].wait_recv()
        z_copies[j].start()
        for d in range(STEP * j, STEP * (j + 1)):
            pass_on(both.at[home], d, slot_h, 0)
    table(0, keep, slot_h, 0, BLOCKS)
    for j in range(CHUNKS):
        z_copies[j].wait_recv()
        for d in range(STEP * j, STEP * (j + 1)):
            pass_on(far, d, slot_f, 1)
        table(0, distant, slot_f, STEP * j, STEP)
    cost_b[cid, slot_h] = both[home, cid]
    cost_b[cid, slot_f] = far[cid]

    def top_first():
        c, s = half[0, 0], half[0, 1]

        def rows(r, carry):
            at = pl.ds(pl.multiple_of(r * 8, 8), 8)
            vals = [(tab[0, k, at, 0:128], -tab[0, k, at, 128:256]) for k in range(BLOCKS)]
            vals = gates(vals, c, s)
            for k in range(BLOCKS):
                work[k, at, 0:128] = vals[k][0]
                work[k, at, 128:256] = vals[k][1]
            return carry

        lax.fori_loop(0, ROWS // 8, rows, 0)

    def top(layer):
        c0, s0, c1, s1 = half[layer - 1, 0], half[layer - 1, 1], half[layer, 0], half[layer, 1]

        def rows(r, carry):
            at = pl.ds(pl.multiple_of(r * 8, 8), 8)
            vals = [(rcv[layer - 1, k, at, 0:128], rcv[layer - 1, k, at, 128:256]) for k in range(BLOCKS)]
            vals = gates(vals, c0, s0)
            for k in range(BLOCKS):
                re, im = vals[k]
                pc, ps = tab[layer, k, at, 0:128], tab[layer, k, at, 128:256]
                vals[k] = (re * pc + im * ps, im * pc - re * ps)
            vals = gates(vals, c1, s1)
            for k in range(BLOCKS):
                work[k, at, 0:128] = vals[k][0]
                work[k, at, 128:256] = vals[k][1]
            return carry

        lax.fori_loop(0, ROWS // 8, rows, 0)

    def low(layer, index):
        xs = jnp.concatenate([work[k] for k in index], axis=0)
        ys = jnp.dot(xs, mix[layer], precision=HIGHEST, preferred_element_type=jnp.float32)
        ys = jnp.concatenate(
            [jnp.concatenate([ys[i * 128:(i + 1) * 128, 0:128].T, ys[i * 128:(i + 1) * 128, 128:256].T], axis=1)
             for i in range(len(index))], axis=0)
        return jnp.dot(ys, mix[layer], precision=HIGHEST, preferred_element_type=jnp.float32)

    def low_and_send(layer):
        started = []
        for group in GROUPS:
            index = [cube_peer(mask)[0] for mask in group]
            ys = low(layer, index)
            for i, mask in enumerate(group):
                if mask:
                    snd[layer, index[i]] = ys[i * 128:(i + 1) * 128]
                else:
                    rcv[layer, cid] = ys[i * 128:(i + 1) * 128]
            for i, mask in enumerate(group):
                if mask:
                    copy = remote(snd.at[layer, index[i]], rcv.at[layer, cid], ss_sem.at[layer, mask],
                                  sr_sem.at[layer, mask], cube_peer(mask)[1])
                    copy.start()
                    started.append(copy)
        return started

    last = LAYERS - 1

    def final_copy(mask):
        b, t, where = plane_peer(mask, h)
        rows = pl.ds(pl.multiple_of(HALF * t, HALF), HALF)
        return [remote(snd.at[last, b + 8 * k, rows], rcv.at[last, cid, HALF * k:HALF * (k + 1)],
                       fs_sem.at[mask, k], fr_sem.at[(mask & 7) + 8 * x, k], where) for k in range(2)]

    def low_and_return():
        for pair in PAIRS:
            index = [plane_peer(mask, h)[0] + 8 * k for mask in pair for k in range(2)]
            ys = low(last, index)
            for i in range(4):
                snd[last, index[i]] = ys[i * 128:(i + 1) * 128]
            for mask in pair:
                for copy in final_copy(mask + 8):
                    copy.start()
        for pair in PAIRS:
            for mask in pair:
                if mask:
                    for copy in final_copy(mask):
                        copy.start()

        @pl.when(home == 0)
        def _():
            for copy in final_copy(0):
                copy.start()

        @pl.when(home == 1)
        def _():
            b = plane_peer(0, h)[0]
            for k in range(2):
                rcv[last, cid, HALF * k:HALF * (k + 1)] = snd[last, b + 8 * k, slot_h]

    top_first()
    pending = low_and_send(0)
    table(2, keep, slot_h, 0, BLOCKS)
    table(2, distant, slot_f, 0, BLOCKS)
    for mask in range(1, BLOCKS):
        peer, where = cube_peer(mask)
        for which, rows in enumerate((slot_h, slot_f)):
            remote(far.at[peer], cost_b.at[peer, rows], cs_sem.at[which, peer], cr_sem.at[which, peer], where).wait()

    def turned(k):
        return cost_b[k].T

    everything = pl.ds(0, ROWS)
    table(1, turned, everything, 0, BLOCKS)
    for layer in range(1, LAYERS):
        if layer == 2:
            table(3, turned, everything, 0, BLOCKS)
        for copy in pending:
            copy.wait()
        top(layer)
        pending = low_and_send(layer) if layer < last else low_and_return()
    for copy in x_copies + z_copies:
        copy.wait_send()
    for mask in range(1, BLOCKS):
        for copy in final_copy(mask):
            copy.wait_send()

    def arrived(m, v):
        for k in range(2):
            remote(snd.at[last, 0, 0:HALF], rcv.at[last, 0, 0:HALF], fs_sem.at[0, k], fr_sem.at[m + 8 * v, k],
                   {'inst': 1 - x, 'qx': qx, 'qy': qy}).wait_recv()

    for m in range(1, 8):
        for v in range(2):
            arrived(m, v)
    arrived(0, 1 - x)

    @pl.when(home == 0)
    def _():
        for copy in final_copy(0):
            copy.wait_send()
        arrived(0, x)

    c, s = half[last, 0], half[last, 1]

    def finish(r, acc):
        at = pl.ds(pl.multiple_of(r * 8, 8), 8)
        vals = gates([(rcv[last, k, at, 0:128], rcv[last, k, at, 128:256]) for k in range(BLOCKS)], c, s)
        for k in range(BLOCKS):
            re, im = vals[k]
            re_ref[k, at, :] = re
            im_ref[k, at, :] = im
            acc = acc + cost_ref[k, at, :] * (re * re + im * im)
        return acc

    me = core + 2 * z0 + 4 * y + 8 * h
    part[me] = lax.fori_loop(0, ROWS // 8, finish, jnp.zeros((8, LANES), jnp.float32))
    sums = [remote(part.at[me], part.at[me], es_sem.at[mask], er_sem.at[mask], plane_peer(mask, x)[2])
            for mask in range(1, BLOCKS)]
    for copy in sums:
        copy.start()
    for copy in sums:
        copy.wait()
    total = part[0]
    for k in range(1, BLOCKS):
        total = total + part[k]
    en_ref[0] = jnp.sum(total) / size


def solution(mesh):
    state_spec = P(('inst', 'qx', 'qy'))

    def device_body(cost_local, gammas, betas):
        local_len = cost_local.shape[0]
        size = local_len * mesh.shape['qx'] * mesh.shape['qy']
        block = (BLOCKS, ROWS, LANES)
        pair = (BLOCKS, ROWS, 2 * LANES)
        vmem = pl.BlockSpec(memory_space=pltpu.VMEM)
        smem = pl.BlockSpec(memory_space=pltpu.SMEM)
        dma = pltpu.SemaphoreType.DMA
        energy, state_re, state_im = pl.pallas_call(
            functools.partial(kernel, size),
            out_shape=(jax.ShapeDtypeStruct((1,), jnp.float32), jax.ShapeDtypeStruct(block, jnp.float32),
                       jax.ShapeDtypeStruct(block, jnp.float32)),
            in_specs=[vmem, smem, smem],
            out_specs=(smem, vmem, vmem),
            scratch_shapes=[
                pltpu.VMEM((2, BLOCKS, HALF, LANES), jnp.float32),
                pltpu.VMEM((BLOCKS, HALF, LANES), jnp.float32),
                pltpu.VMEM(block, jnp.float32),
                pltpu.VMEM(pair, jnp.float32),
                pltpu.VMEM((LAYERS,) + pair, jnp.float32),
                pltpu.VMEM((LAYERS,) + pair, jnp.float32),
                pltpu.VMEM((LAYERS,) + pair, jnp.float32),
                pltpu.VMEM((LAYERS, 2 * LANES, 2 * LANES), jnp.float32),
                pltpu.VMEM((LAYERS, 2, 8, LANES), jnp.float32),
                pltpu.VMEM((BLOCKS, 8, LANES), jnp.float32),
                dma((CHUNKS,)), dma((CHUNKS,)), dma((CHUNKS,)), dma((CHUNKS,)),
                dma((2, BLOCKS)), dma((2, BLOCKS)),
                dma((LAYERS, BLOCKS)), dma((LAYERS, BLOCKS)),
                dma((BLOCKS, 2)), dma((BLOCKS, 2)),
                dma((BLOCKS,)), dma((BLOCKS,)),
            ],
            compiler_params=pltpu.CompilerParams(collective_id=0, has_side_effects=True),
            name='qaoa',
        )(cost_local.reshape(block), gammas, betas)
        return energy, state_re.reshape(local_len), state_im.reshape(local_len)

    return jax.shard_map(device_body, mesh=mesh, in_specs=(state_spec, P(), P()),
                         out_specs=(P('inst'), state_spec, state_spec), check_vma=False)
```
